32 devices in a mesh: fsdp: 8 (over z, y), tp: 4 (over x, core).
Axes of the slice: x: 2, y: 2, z: 4, core: 2. Of those that a mesh axis runs over, the one named last changes fastest.
Arguments:
- audio_codes: int32 [2, 8, 4, 1024], P(None, 'fsdp'), may hold values from 0 to 2047
- text_states: bfloat16 [2, 8, 64, 1024], P(None, 'fsdp'), may hold values from -6 to 6
- clip_weight: int32 [2, 8], P(None, 'fsdp'), may hold values from 0 to 1, as said below
- text_length: int32 [2, 8], P(None, 'fsdp'), may hold values from 1 to 64, as said below
- step_count: int32 [1], replicated, may hold values from 1 to 20
- vocab_tables: float32 [2, 4, 1024, 2048], P(None, None, 'fsdp', 'tp')
- attn_weights: float32 [8, 1024, 1024], P(None, 'fsdp', 'tp')
- ffn_weights: float32 [2, 1024, 4096], P(None, 'fsdp', 'tp'), may hold values from -0.1875 to 0.1875
- norm_params: float32 [8, 1024], P(None, 'fsdp')
- vocab_m: float32 [2, 4, 1024, 2048], P(None, None, 'fsdp', 'tp')
- vocab_v: float32 [2, 4, 1024, 2048], P(None, None, 'fsdp', 'tp')
- attn_m: float32 [8, 1024, 1024], P(None, 'fsdp', 'tp')
- attn_v: float32 [8, 1024, 1024], P(None, 'fsdp', 'tp')
- ffn_m: float32 [2, 1024, 4096], P(None, 'fsdp', 'tp')
- ffn_v: float32 [2, 1024, 4096], P(None, 'fsdp', 'tp')
- norm_m: float32 [8, 1024], P(None, 'fsdp')
- norm_v: float32 [8, 1024], P(None, 'fsdp')
Outputs:
- step_loss: float32 [], replicated
- grad_norm: float32 [], replicated
- vocab_new: float32 [2, 4, 1024, 2048], P(None, None, 'fsdp', 'tp')
- vocab_m_new: float32 [2, 4, 1024, 2048], P(None, None, 'fsdp', 'tp')
- vocab_v_new: float32 [2, 4, 1024, 2048], P(None, None, 'fsdp', 'tp')
- vocab_low: bfloat16 [2, 4, 1024, 2048], P(None, None, 'fsdp', 'tp')
- attn_new: float32 [8, 1024, 1024], P(None, 'fsdp', 'tp')
- attn_m_new: float32 [8, 1024, 1024], P(None, 'fsdp', 'tp')
- attn_v_new: float32 [8, 1024, 1024], P(None, 'fsdp', 'tp')
- attn_low: bfloat16 [8, 1024, 1024], P(None, 'fsdp', 'tp')
- ffn_new: float32 [2, 1024, 4096], P(None, 'fsdp', 'tp')
- ffn_m_new: float32 [2, 1024, 4096], P(None, 'fsdp', 'tp')
- ffn_v_new: float32 [2, 1024, 4096], P(None, 'fsdp', 'tp')
- ffn_low: bfloat16 [2, 1024, 4096], P(None, 'fsdp', 'tp')
- norm_new: float32 [8, 1024], P(None, 'fsdp')
- norm_m_new: float32 [8, 1024], P(None, 'fsdp')
- norm_v_new: float32 [8, 1024], P(None, 'fsdp')
- norm_low: bfloat16 [8, 1024], P(None, 'fsdp')
The draws below stay inside these ranges and needn't reach their ends.
Inputs may be any that keep to these rules, and one draw needn't show every extreme that they name: `clip_weight`: the first slot of the first micro-batch holds a clip. `text_length`: the first slot of the first micro-batch has all 64 text states.
All inputs are finite; a program needn't handle non-finite values.
Results may differ from the reference program's by a relative error of at most 0.002.
The reference program's roundings to bfloat16 on the way count: a program that leaves them out, or rounds other values in their place, can miss the bound.
Values may be sent and summed in bfloat16 or wider, within the bound.
A program may use at most 184 MiB of HBM per device.

```python
import math
import jax
import jax.numpy as jnp
from jax import lax

D = 1024
HEADS = 16
HEAD_DIM = 64
FF = 4096
VOCAB = 2048
BOOKS = 4
TEXT = 64
FRAMES = 1024
MICRO = 2
CLIPS = 8
PARAMS = 33562624


def moment_scale():
    counted = CLIPS * MICRO * BOOKS * (FRAMES - 1) * 2.0 / 3.0
    return 24.0 * math.sqrt(counted / PARAMS)


def first_moment(key, shape):
    return 0.11 * moment_scale() * jax.random.normal(key, shape, jnp.float32)


def second_moment(key, shape):
    spread = jax.random.uniform(key, shape, jnp.float32, math.log(0.3), math.log(3.0))
    scale_value = moment_scale()
    return 0.053 * scale_value * scale_value * jnp.exp(spread)


def draw_clip_weight(key, part):
    picks = jax.random.randint(key, (MICRO, CLIPS), 0, 3)
    live_mask = (picks > 0).astype(jnp.int32)
    return live_mask.at[0, 0].set(1)


def draw_text_length(key, part):
    lengths = jax.random.randint(key, (MICRO, CLIPS), 1, TEXT + 1)
    return lengths.at[0, 0].set(TEXT)


def draw_vocab_tables(key, part):
    noise_draw = jax.random.normal(key, (2, BOOKS, D, VOCAB), jnp.float32)
    scales = jnp.array([0.25, 2.0 / math.sqrt(D)], jnp.float32)
    return noise_draw * scales[:, None, None, None]


def draw_attn_weights(key, part):
    noise_draw = jax.random.normal(key, (8, D, D), jnp.float32)
    scales = jnp.array([1.0, 1.0, 1.0, 1.0, 1.0, 1.0, 8.0, 4.0], jnp.float32) / math.sqrt(D)
    return noise_draw * scales[:, None, None]


def draw_norm_params(key, part):
    key_one, key_two = jax.random.split(key)
    gains = jax.random.uniform(key_one, (4, D), jnp.float32, 0.5, 1.5)
    shifts = 0.3 * jax.random.normal(key_two, (4, D), jnp.float32)
    return jnp.concatenate([gains, shifts], axis=0)


def draw_vocab_m(key, part):
    return first_moment(key, (2, BOOKS, D, VOCAB))


def draw_vocab_v(key, part):
    return second_moment(key, (2, BOOKS, D, VOCAB))


def draw_attn_m(key, part):
    return first_moment(key, (8, D, D))


def draw_attn_v(key, part):
    return second_moment(key, (8, D, D))


def draw_ffn_m(key, part):
    return first_moment(key, (2, D, FF))


def draw_ffn_v(key, part):
    return second_moment(key, (2, D, FF))


def draw_norm_m(key, part):
    return first_moment(key, (8, D))


def draw_norm_v(key, part):
    return second_moment(key, (8, D))


def touch_ends(values, rng, least, largest):
    spot = [jax.random.randint(jax.random.fold_in(rng, axis), (), 0, length) for axis, length in enumerate(values.shape)]
    longest = values.shape.index(max(values.shape))
    beside = spot[:longest] + [(spot[longest] + 1) % values.shape[longest]] + spot[longest + 1:]
    return values.at[tuple(spot)].set(least).at[tuple(beside)].set(largest)


def levels(stream_key, extent, pieces, low, high):
    def one(axis_at, blocks):
        steps = jax.random.uniform(jax.random.fold_in(jax.random.fold_in(stream_key, 6), axis_at), (blocks,), jnp.float32, low / len(pieces), high / len(pieces))
        return jnp.repeat(jnp.exp(steps), extent[axis_at] // blocks).reshape((-1,) + (1,) * (len(extent) - axis_at - 1))

    factor_of = one(*pieces[0])
    for cut in pieces[1:]:
        factor_of = factor_of * one(*cut)
    return factor_of


def noise(own_key, extent, deviation, most, pieces=(), held_as=jnp.bfloat16):
    entries = deviation * jax.random.normal(own_key, extent, jnp.float32)
    if pieces:
        entries = entries * levels(own_key, extent, pieces, -0.22, 0.18)
    return jnp.clip(entries, -most, most).astype(held_as)


def setup_inputs(seed: int = 0) -> dict:
    key_of = jax.random.split(jax.random.key(seed), 18)
    return {
        "audio_codes": touch_ends(jax.random.randint(key_of[0], (MICRO, CLIPS, BOOKS, FRAMES), 0, VOCAB), jax.random.fold_in(key_of[0], 1), 0, VOCAB - 1).astype(jnp.int32),
        "text_states": noise(key_of[1], (MICRO, CLIPS, TEXT, D), 1.0, 6.0, ((1, 8),)),
        "clip_weight": draw_clip_weight(jax.random.fold_in(key_of[17], 71), 0),
        "text_length": draw_text_length(jax.random.fold_in(key_of[17], 71), 0),
        "step_count": jax.random.randint(key_of[4], (1,), 1, 21).astype(jnp.int32),
        "vocab_tables": draw_vocab_tables(jax.random.fold_in(key_of[17], 71), 0),
        "attn_weights": draw_attn_weights(jax.random.fold_in(key_of[17], 71), 0),
        "ffn_weights": noise(key_of[7], (2, D, FF), D ** -0.5, 0.1875, ((1, 8), (2, 4)), jnp.float32),
        "norm_params": draw_norm_params(jax.random.fold_in(key_of[17], 71), 0),
        "vocab_m": draw_vocab_m(jax.random.fold_in(key_of[17], 71), 0),
        "vocab_v": draw_vocab_v(jax.random.fold_in(key_of[17], 71), 0),
        "attn_m": draw_attn_m(jax.random.fold_in(key_of[17], 71), 0),
        "attn_v": draw_attn_v(jax.random.fold_in(key_of[17], 71), 0),
        "ffn_m": draw_ffn_m(jax.random.fold_in(key_of[17], 71), 0),
        "ffn_v": draw_ffn_v(jax.random.fold_in(key_of[17], 71), 0),
        "norm_m": draw_norm_m(jax.random.fold_in(key_of[17], 71), 0),
        "norm_v": draw_norm_v(jax.random.fold_in(key_of[17], 71), 0),
    }


@jax.custom_vjp
def low(v):
    return lax.optimization_barrier(v.astype(jnp.bfloat16)).astype(jnp.float32)

@jax.custom_vjp
def low_back(v):
    return v

def low_keep(v):
    return (low(v), None)

def low_pass(kept, grad):
    return (grad,)

def back_keep(v):
    return (v, None)

def back_low(kept, grad):
    return (low(grad),)
low.defvjp(low_keep, low_pass)
low_back.defvjp(back_keep, back_low)
ln_eps = 1e-05
smooth = 0.1
z_weight = 0.01
clip_scale = 24.0
learn_rate = 0.02
beta_one = 0.9
beta_two = 0.95
adam_eps = 1e-08
weight_decay = 0.1
neg_big = -1e+30
highest = lax.Precision.HIGHEST

def product_of(left, right):
    return jnp.dot(left, right, precision=highest, preferred_element_type=jnp.float32)

def layer_norm(values, gain_row, shift_row):
    centred = values - lax.optimization_barrier(jnp.mean(values, axis=-1, keepdims=True))
    spread = lax.optimization_barrier(jnp.mean(centred * centred, axis=-1, keepdims=True))
    return centred * lax.rsqrt(spread + ln_eps) * gain_row + shift_row

def positions(first_row, row_count, model_width):
    half_width = model_width // 2
    steps = jnp.arange(half_width).astype(jnp.float32)
    frequencies = jnp.exp(-math.log(10000.0) * steps / (half_width - 1))
    places = (first_row + jnp.arange(row_count)).astype(jnp.float32)
    angles = places[:, None] * frequencies[None, :]
    return jnp.concatenate([jnp.cos(angles), jnp.sin(angles)], axis=1)

def softmax_rows(scores):
    row_top = lax.optimization_barrier(jnp.max(scores, axis=-1, keepdims=True))
    exp_scores = jnp.exp(scores - row_top)
    return exp_scores / lax.optimization_barrier(jnp.sum(exp_scores, axis=-1, keepdims=True))

def attend(queries, key_rows, values, allowed, score_scale):
    frames = queries.shape[0]
    span = key_rows.shape[0]
    query_heads = queries.reshape(frames, HEADS, HEAD_DIM)
    key_heads = key_rows.reshape(span, HEADS, HEAD_DIM)
    value_heads = values.reshape(span, HEADS, HEAD_DIM)
    scores = low_back(jnp.einsum('qhd,khd->hqk', query_heads, key_heads, precision=highest) * score_scale)
    scores = jnp.where(allowed[None], scores, neg_big)
    weights = low(softmax_rows(scores))
    mixed_heads = jnp.einsum('hqk,khd->qhd', weights, value_heads, precision=highest)
    return low_back(low(mixed_heads.reshape(frames, D)))

def clip_loss(weights, clip_codes, clip_text, clip_live, clip_span):
    vocab, attn, ffn, norms = weights
    score_scale = HEAD_DIM ** (-0.5)
    frame_ids = jnp.arange(FRAMES)
    book_ids = jnp.arange(BOOKS)[:, None]
    live_mask = frame_ids[None, :] >= book_ids
    counted = (live_mask & (frame_ids[None, :] <= FRAMES - 2)).astype(jnp.float32)
    embedded = jnp.zeros((FRAMES, D), jnp.float32)
    for book_index in range(BOOKS):
        table_rows = jnp.take(vocab[0, book_index].T, clip_codes[book_index], axis=0)
        embedded = embedded + jnp.where(live_mask[book_index][:, None], table_rows, 0.0)
    residual = low_back(embedded) + positions(0, FRAMES, D)
    causal = frame_ids[:, None] >= frame_ids[None, :]
    normed = low(layer_norm(residual, norms[0], norms[4]))
    queries = low_back(low(product_of(normed, attn[0])))
    key_rows = low_back(low(product_of(normed, attn[1])))
    values = low_back(low(product_of(normed, attn[2])))
    mixed_heads = attend(queries, key_rows, values, causal, score_scale)
    residual = residual + low_back(product_of(mixed_heads, attn[6].T))
    normed = low(layer_norm(residual, norms[1], norms[5]))
    queries = low_back(low(product_of(normed, attn[3])))
    key_rows = low_back(low(product_of(clip_text, attn[4])))
    values = low_back(low(product_of(clip_text, attn[5])))
    allowed = jnp.broadcast_to(jnp.arange(TEXT)[None, :] < clip_span, (FRAMES, TEXT))
    mixed_heads = attend(queries, key_rows, values, allowed, score_scale)
    residual = residual + low_back(product_of(mixed_heads, attn[7].T))
    normed = low(layer_norm(residual, norms[2], norms[6]))
    hidden_pre = low_back(product_of(normed, ffn[0]))
    active = low(jax.nn.gelu(hidden_pre, approximate=False))
    residual = residual + low_back(product_of(active, ffn[1].T))
    normed = low(layer_norm(residual, norms[3], norms[7]))
    logits = low_back(jnp.einsum('fd,kdv->kfv', normed, vocab[1], precision=highest))
    row_top = lax.optimization_barrier(jnp.max(logits, axis=-1))
    log_total = jnp.log(lax.optimization_barrier(jnp.sum(jnp.exp(logits - row_top[..., None]), axis=-1))) + row_top
    target = jnp.concatenate([clip_codes[:, 1:], jnp.zeros((BOOKS, 1), jnp.int32)], axis=1)
    picked = jnp.take_along_axis(logits, target[..., None], axis=-1)[..., 0]
    average = lax.optimization_barrier(jnp.mean(logits, axis=-1))
    loss_terms = log_total - (1.0 - smooth) * picked - smooth * average + z_weight * log_total * log_total
    return clip_live * jnp.sum(loss_terms * counted)

def adam_update(master, gradient, moment_one, moment_two, factor, step_float, decayed):
    clipped = gradient * factor
    moment_one = beta_one * moment_one + (1.0 - beta_one) * clipped
    moment_two = beta_two * moment_two + (1.0 - beta_two) * clipped * clipped
    fix_one = 1.0 - jnp.power(beta_one, step_float)
    fix_two = 1.0 - jnp.power(beta_two, step_float)
    change = moment_one / fix_one / (jnp.sqrt(moment_two / fix_two) + adam_eps)
    if decayed:
        change = change + weight_decay * master
    updated = master - learn_rate * change
    return (updated, moment_one, moment_two, updated.astype(jnp.bfloat16))

def reference(audio_codes, text_states, clip_weight, text_length, step_count, vocab_tables, attn_weights, ffn_weights, norm_params, vocab_m, vocab_v, attn_m, attn_v, ffn_m, ffn_v, norm_m, norm_v):
    masters = (vocab_tables, attn_weights, ffn_weights, norm_params)
    flat_codes = audio_codes.reshape(MICRO * CLIPS, BOOKS, FRAMES)
    flat_text = text_states.astype(jnp.float32).reshape(MICRO * CLIPS, TEXT, D)
    flat_live = clip_weight.reshape(MICRO * CLIPS).astype(jnp.float32)
    flat_span = text_length.reshape(MICRO * CLIPS)
    clip_fn = jax.checkpoint(clip_loss)

    def objective(weights):
        rounded = tuple((low(item) for item in weights))

        def add_clip(carry, item):
            clip_codes, clip_text, clip_live, clip_span = item
            return (carry + clip_fn(rounded, clip_codes, clip_text, clip_live, clip_span), None)
        summed, _ = lax.scan(add_clip, jnp.zeros((), jnp.float32), (flat_codes, flat_text, flat_live, flat_span))
        return summed
    summed, pullback = jax.vjp(objective, masters)
    grads = pullback(jnp.ones((), jnp.float32))[0]
    per_clip = BOOKS * (FRAMES - 1) - BOOKS * (BOOKS - 1) // 2
    counted_total = jnp.sum(clip_weight).astype(jnp.float32) * per_clip
    step_loss = summed / counted_total
    squares = jnp.zeros((), jnp.float32)
    for gradient in grads:
        squares = squares + jnp.sum(gradient * gradient)
    grad_norm = jnp.sqrt(squares)
    factor = jnp.minimum(1.0, clip_scale * jnp.sqrt(counted_total) / (grad_norm + 1e-06))
    step_float = step_count[0].astype(jnp.float32)
    vocab_out = adam_update(vocab_tables, grads[0], vocab_m, vocab_v, factor, step_float, True)
    attn_out = adam_update(attn_weights, grads[1], attn_m, attn_v, factor, step_float, True)
    ffn_out = adam_update(ffn_weights, grads[2], ffn_m, ffn_v, factor, step_float, True)
    norm_out = adam_update(norm_params, grads[3], norm_m, norm_v, factor, step_float, False)
    return (step_loss, grad_norm, vocab_out[0], vocab_out[1], vocab_out[2], vocab_out[3], attn_out[0], attn_out[1], attn_out[2], attn_out[3], ffn_out[0], ffn_out[1], ffn_out[2], ffn_out[3], norm_out[0], norm_out[1], norm_out[2], norm_out[3])
```

```python
import math

import jax
import jax.numpy as jnp
from jax import lax
from jax.sharding import PartitionSpec as P

D = 1024
HEAD_DIM = 64
VOCAB = 2048
BOOKS = 4
MICRO = 2

ln_eps = 1e-05
smooth = 0.1
z_weight = 0.01
clip_scale = 24.0
learn_rate = 0.02
beta_one = 0.9
beta_two = 0.95
adam_eps = 1e-08
weight_decay = 0.1
neg_big = -1e30


bf16 = jnp.bfloat16
f32 = jnp.float32


def mm(spec, left, right):
    return jnp.einsum(spec, left, right, preferred_element_type=f32)


def fsdp_levels():
    left = lax.axis_size("fsdp")
    levels, stride = [], 1
    for size in (2,) + (4,) * 8:
        size = min(size, left)
        if size == 1:
            break
        levels.append((size, stride))
        stride *= size
        left //= size
    return levels


def shifted(index, size, stride, shift):
    digit = index // stride % size
    return index + ((digit + shift) % size - digit) * stride


def fsdp_shift(value, size, stride, shift):
    count = lax.axis_size("fsdp")
    return lax.ppermute(value, "fsdp", [(i, shifted(i, size, stride, shift)) for i in range(count)])


def block_owners(index):
    owners = [index]
    for size, stride in reversed(fsdp_levels()):
        owners = [shifted(o, size, stride, -s) for s in range(size) for o in owners]
    return owners


def fsdp_gather(shard, axis):
    held = shard
    for size, stride in reversed(fsdp_levels()):
        parts = [held] + [fsdp_shift(held, size, stride, s) for s in range(1, size)]
        held = jnp.concatenate(parts, axis=axis)
    return held


def fsdp_scatter(total, axis):
    for size, stride in fsdp_levels():
        parts = jnp.split(total, size, axis=axis)
        total = parts[0]
        for s in range(1, size):
            total = total + fsdp_shift(parts[s], size, stride, -s)
    return total


def tp_swap(value, bit):
    return lax.ppermute(value, "tp", [(i, i ^ bit) for i in range(lax.axis_size("tp"))])


def row_swap(value, bit):
    blocks = jnp.split(tp_swap(value, bit), lax.axis_size("tp"), axis=-1)
    order = tp_order()
    return jnp.concatenate([blocks[order.index(o ^ bit)] for o in order], axis=-1)


def tp_bits():
    return [1 << b for b in range(lax.axis_size("tp").bit_length() - 1)]


def tp_order():
    order = [0]
    for bit in reversed(tp_bits()):
        order = order + [o ^ bit for o in order]
    return order


def full_rows(row_block):
    held = [row_block]
    for bit in reversed(tp_bits()):
        held = held + [tp_swap(h, bit) for h in held]
    return jnp.concatenate(held, axis=0)


def row_sums(product, left):
    half = left.shape[-2] // 2
    sent = product(left[..., half:, :])
    kept = product(left[..., :half, :])
    total = kept + tp_swap(sent, 1)
    for bit in tp_bits()[1:]:
        half = total.shape[0] // 2
        total = total[:half] + tp_swap(total[half:], bit)
    return total


def layer_norm(values, gain_row, shift_row):
    centred = values - jnp.mean(values, axis=-1, keepdims=True)
    spread = jnp.mean(centred * centred, axis=-1, keepdims=True)
    return centred * lax.rsqrt(spread + ln_eps) * gain_row + shift_row


def norm_back(values, gain_row, gradient):
    centred = values - jnp.mean(values, axis=-1, keepdims=True)
    scale = lax.rsqrt(jnp.mean(centred * centred, axis=-1, keepdims=True) + ln_eps)
    normed = centred * scale
    scaled = gradient * gain_row
    step = scale * (
        scaled
        - jnp.mean(scaled, axis=-1, keepdims=True)
        - normed * jnp.mean(scaled * normed, axis=-1, keepdims=True)
    )
    return step, jnp.sum(gradient * normed, axis=0), jnp.sum(gradient, axis=0)


def exact_gelu(values):
    return jax.nn.gelu(values, approximate=False)


def gelu_back(values, gradient):
    _, pullback = jax.vjp(exact_gelu, values)
    return pullback(gradient)[0]


def positions(first_row, row_count, model_width):
    half_width = model_width // 2
    steps = jnp.arange(half_width).astype(f32)
    frequencies = jnp.exp(-math.log(10000.0) * steps / (half_width - 1))
    places = (first_row + jnp.arange(row_count)).astype(f32)
    angles = places[:, None] * frequencies[None, :]
    return jnp.concatenate([jnp.cos(angles), jnp.sin(angles)], axis=1)


def merge_stats(earlier, later):
    row_top = jnp.maximum(earlier[0], later[0])
    row_mass = earlier[1] * jnp.exp(earlier[0] - row_top) + later[1] * jnp.exp(later[0] - row_top)
    return jnp.stack([row_top, row_mass, earlier[2] + later[2], earlier[3] + later[3]])


def split_heads(values):
    return values.reshape(values.shape[0], values.shape[1] // HEAD_DIM, HEAD_DIM)


def masked_scores(queries, key_rows, allowed, score_scale):
    scores = mm("qhd,khd->hqk", split_heads(queries), split_heads(key_rows)) * score_scale
    return jnp.where(allowed[None], scores, neg_big)


def attend_forward(queries, key_rows, values, allowed, score_scale):
    scores = masked_scores(queries, key_rows, allowed, score_scale)
    row_top = jnp.max(scores, axis=-1, keepdims=True)
    exp_scores = jnp.exp(scores - row_top)
    row_mass = jnp.sum(exp_scores, axis=-1, keepdims=True)
    weights = (exp_scores / row_mass).astype(bf16)
    mixed_heads = mm("hqk,khd->qhd", weights, split_heads(values))
    return (mixed_heads.reshape(queries.shape).astype(bf16), row_top + jnp.log(row_mass))


def attend_backward(queries, key_rows, values, allowed, score_scale, summary, grad_mixed):
    scores = masked_scores(queries, key_rows, allowed, score_scale)
    prob_rows = jnp.exp(scores - summary)
    grad_heads = split_heads(grad_mixed)
    grad_values = mm("hqk,qhd->khd", prob_rows.astype(bf16), grad_heads)
    grad_probs = mm("qhd,khd->hqk", grad_heads, split_heads(values))
    inner_sum = jnp.sum(prob_rows * grad_probs, axis=-1, keepdims=True)
    grad_scores = (prob_rows * (grad_probs - inner_sum)).astype(bf16)
    grad_queries = mm("hqk,khd->qhd", grad_scores, split_heads(key_rows)) * score_scale
    grad_keys = mm("hqk,qhd->khd", grad_scores, split_heads(queries)) * score_scale
    return (
        grad_queries.reshape(queries.shape).astype(bf16),
        grad_keys.reshape(key_rows.shape).astype(bf16),
        grad_values.reshape(values.shape).astype(bf16),
    )


def adam_update(master, gradient, moment_one, moment_two, factor, step_float, decayed):
    clipped = gradient * factor
    moment_one = beta_one * moment_one + (1.0 - beta_one) * clipped
    moment_two = beta_two * moment_two + (1.0 - beta_two) * clipped * clipped
    fix_one = 1.0 - jnp.power(beta_one, step_float)
    fix_two = 1.0 - jnp.power(beta_two, step_float)
    change = moment_one / fix_one / (jnp.sqrt(moment_two / fix_two) + adam_eps)
    if decayed:
        change = change + weight_decay * master
    updated = master - learn_rate * change
    return (updated, moment_one, moment_two, updated.astype(bf16))


def after(value, *earlier):
    return lax.optimization_barrier((value,) + earlier)[0]


class Kept:
    pass


def per_device(
    audio_codes,
    text_states,
    clip_weight,
    text_length,
    step_count,
    vocab_tables,
    attn_weights,
    ffn_weights,
    norm_params,
    vocab_m,
    vocab_v,
    attn_m,
    attn_v,
    ffn_m,
    ffn_v,
    norm_m,
    norm_v,
):
    tp_count = lax.axis_size("tp")
    fsdp_count = lax.axis_size("fsdp")
    tp_index = lax.axis_index("tp")
    fsdp_index = lax.axis_index("fsdp")
    frames = audio_codes.shape[3]
    local_rows = frames // tp_count
    shard_rows = D // fsdp_count
    vocab_local = vocab_tables.shape[3]
    head_cols = attn_weights.shape[2]
    score_scale = HEAD_DIM ** (-0.5)

    owners = block_owners(fsdp_index)

    def own_columns(values):
        return jnp.concatenate(
            [lax.dynamic_slice_in_dim(values, o * shard_rows, shard_rows, axis=-1) for o in owners],
            axis=-1,
        )

    places = [tp_index ^ o for o in tp_order()]

    def own_frames(values):
        return jnp.concatenate(
            [lax.dynamic_slice_in_dim(values, p * local_rows, local_rows, axis=-1) for p in places],
            axis=-1,
        )

    table_low = vocab_tables.astype(bf16)
    attn_low = attn_weights.astype(bf16)
    norm_low = jnp.pad(norm_params.astype(bf16).T, ((0, 0), (0, head_cols - 8)))
    first_half = fsdp_gather(table_low[0, :2], 1)
    second_half = fsdp_gather(after(table_low[0, 2:], first_half), 1)
    self_shard = jnp.concatenate([attn_low[0:3], attn_low[6:7], norm_low[None]], axis=0)
    self_full = fsdp_gather(after(self_shard, second_half), 1)
    cross_shard = jnp.concatenate([attn_low[3:6], attn_low[7:8]], axis=0)
    cross_full = fsdp_gather(after(cross_shard, self_full), 1)
    ffn_full = fsdp_gather(after(ffn_weights.astype(bf16), cross_full), 1)
    head_full = fsdp_gather(after(table_low[1], ffn_full), 1)
    tables = (first_half, second_half)
    gains = self_full[4, :, :8].T.astype(f32)
    in_self, out_self = self_full[0:3], self_full[3]
    in_query, in_text, out_cross = cross_full[0], cross_full[1:3], cross_full[3]
    up, down = ffn_full[0], ffn_full[1]

    place_rows = own_columns(positions(tp_index * local_rows, local_rows, D))
    text_rows = own_columns(text_states[:, 0])
    frame_ids = own_frames(jnp.arange(frames))
    causal = frame_ids[:, None] >= frame_ids[None, :]
    book_ids = jnp.arange(BOOKS)[:, None]
    live_mask = frame_ids[None, :] >= book_ids
    counted = (live_mask & (frame_ids[None, :] <= frames - 2)).astype(f32)
    vocab_ids = jnp.arange(vocab_local)
    text_ids = jnp.arange(text_states.shape[2])

    def forward(m):
        kept = Kept()
        codes = own_frames(audio_codes[m, 0])
        targets = own_frames(
            jnp.concatenate(
                [audio_codes[m, 0][:, 1:], jnp.zeros((BOOKS, 1), jnp.int32)], axis=1
            )
        )
        live = clip_weight[m, 0].astype(f32)
        allowed = jnp.broadcast_to(
            text_ids[None, :] < text_length[m, 0], (frames, text_ids.shape[0])
        )
        local_ids = codes - tp_index * vocab_local
        one_hot = (
            (local_ids[:, :, None] == vocab_ids) & live_mask[:, :, None]
        ).astype(bf16)
        embedded = row_sums(
            lambda rows: mm("kfv,kdv->fd", rows[:2], tables[0])
            + mm("kfv,kdv->fd", rows[2:], tables[1]),
            one_hot,
        )
        state_zero = embedded + place_rows
        rows_one = full_rows(layer_norm(state_zero, gains[0], gains[4]).astype(bf16))
        self_proj = mm("fd,jde->jfe", rows_one, in_self).astype(bf16)
        mixed_one, summary_one = attend_forward(
            self_proj[0], self_proj[1], self_proj[2], causal, score_scale
        )
        state_one = state_zero + row_sums(lambda o: mm("fe,de->fd", o, out_self), mixed_one)
        rows_two = full_rows(layer_norm(state_one, gains[1], gains[5]).astype(bf16))
        cross_query = mm("fd,de->fe", rows_two, in_query).astype(bf16)
        cross_kv = mm("td,jde->jte", text_rows[m], in_text).astype(bf16)
        mixed_two, summary_two = attend_forward(
            cross_query, cross_kv[0], cross_kv[1], allowed, score_scale
        )
        state_two = state_one + row_sums(lambda o: mm("fe,de->fd", o, out_cross), mixed_two)
        rows_three = full_rows(layer_norm(state_two, gains[2], gains[6]).astype(bf16))
        hidden_pre = mm("fd,de->fe", rows_three, up)
        active = exact_gelu(hidden_pre).astype(bf16)
        state_three = state_two + row_sums(lambda o: mm("fe,de->fd", o, down), active)
        rows_four = full_rows(layer_norm(state_three, gains[3], gains[7]).astype(bf16))
        logits = mm("fd,kdv->kfv", rows_four, head_full)
        row_top = jnp.max(logits, axis=-1)
        row_mass = jnp.sum(jnp.exp(logits - row_top[..., None]), axis=-1)
        chosen = (targets - tp_index * vocab_local)[..., None] == vocab_ids
        picked = jnp.sum(jnp.where(chosen, logits, 0.0), axis=-1)
        summed = jnp.sum(logits, axis=-1)
        stats = jnp.stack([row_top, row_mass, picked, summed])
        for bit in tp_bits():
            stats = merge_stats(stats, row_swap(stats, bit))
        log_total = stats[0] + jnp.log(stats[1])
        loss_terms = (
            log_total
            - (1.0 - smooth) * stats[2]
            - smooth * stats[3] / VOCAB
            + z_weight * log_total * log_total
        )
        numerator = live * jnp.sum(loss_terms * counted)
        row_scale = (live * counted)[..., None]
        prob_rows = jnp.exp(logits - log_total[..., None])
        grad_logits = (
            row_scale
            * (
                prob_rows * (1.0 + 2.0 * z_weight * log_total[..., None])
                - (1.0 - smooth) * chosen.astype(f32)
                - smooth / VOCAB
            )
        ).astype(bf16)
        kept.__dict__.update(locals())
        return kept

    def head_back(k):
        grad_rows = row_sums(lambda g: mm("kfv,kdv->fd", g, head_full), k.grad_logits)
        k.grad_head = mm("kfv,fd->kdv", k.grad_logits, k.rows_four)
        k.grad_state, k.gain_four, k.shift_four = norm_back(
            k.state_three, gains[3], grad_rows
        )

    def ffn_back(k):
        grad_out = full_rows(k.grad_state.astype(bf16))
        k.grad_down = mm("fe,fd->de", k.active, grad_out)
        grad_active = mm("fd,de->fe", grad_out, down)
        grad_hidden = gelu_back(k.hidden_pre, grad_active).astype(bf16)
        k.grad_up = mm("fe,fd->de", grad_hidden, k.rows_three)
        step, k.gain_three, k.shift_three = norm_back(
            k.state_two, gains[2], row_sums(lambda g: mm("fe,de->fd", g, up), grad_hidden)
        )
        k.grad_state = k.grad_state + step

    def cross_back(k):
        grad_out = full_rows(k.grad_state.astype(bf16))
        grad_cross_out = mm("fe,fd->de", k.mixed_two, grad_out)
        grad_mixed = mm("fd,de->fe", grad_out, out_cross).astype(bf16)
        grad_cq, grad_ck, grad_cv = attend_backward(
            k.cross_query,
            k.cross_kv[0],
            k.cross_kv[1],
            k.allowed,
            score_scale,
            k.summary_two,
            grad_mixed,
        )
        text = text_rows[k.m]
        k.grad_cross = [
            mm("fe,fd->de", grad_cq, k.rows_two),
            mm("te,td->de", grad_ck, text),
            mm("te,td->de", grad_cv, text),
            grad_cross_out,
        ]
        step, k.gain_two, k.shift_two = norm_back(
            k.state_one, gains[1], row_sums(lambda g: mm("fe,de->fd", g, in_query), grad_cq)
        )
        k.grad_state = k.grad_state + step

    def self_back(k):
        grad_out = full_rows(k.grad_state.astype(bf16))
        grad_self_out = mm("fe,fd->de", k.mixed_one, grad_out)
        grad_mixed = mm("fd,de->fe", grad_out, out_self).astype(bf16)
        grads = attend_backward(
            k.self_proj[0],
            k.self_proj[1],
            k.self_proj[2],
            causal,
            score_scale,
            k.summary_one,
            grad_mixed,
        )
        grad_self = jnp.stack(grads)
        k.grad_self = [mm("fe,fd->de", g, k.rows_one) for g in grads] + [grad_self_out]
        step, k.gain_one, k.shift_one = norm_back(
            k.state_zero,
            gains[0],
            row_sums(lambda g: mm("jfe,jde->fd", g, in_self), grad_self),
        )
        k.grad_state = k.grad_state + step

    def embed_back(k):
        grad_embed = full_rows(k.grad_state.astype(bf16))
        k.grad_table = mm("kfv,fd->kdv", k.one_hot, grad_embed)

    clips = [forward(m) for m in range(MICRO)]
    for stage in (head_back, ffn_back, cross_back, self_back, embed_back):
        for k in clips:
            stage(k)

    one, two = clips
    head_shard = fsdp_scatter(one.grad_head + two.grad_head, 1)
    up_shard = fsdp_scatter(one.grad_up + two.grad_up, 0)
    down_shard = fsdp_scatter(one.grad_down + two.grad_down, 0)
    cross_shards = fsdp_scatter(jnp.stack([a + b for a, b in zip(one.grad_cross, two.grad_cross)]), 1)
    self_shards = fsdp_scatter(jnp.stack([a + b for a, b in zip(one.grad_self, two.grad_self)]), 1)
    table_shard = fsdp_scatter(one.grad_table + two.grad_table, 1)

    def norm_sums(k):
        return jnp.stack(
            [k.gain_one, k.gain_two, k.gain_three, k.gain_four]
            + [k.shift_one, k.shift_two, k.shift_three, k.shift_four]
        )

    gain_total = norm_sums(one) + norm_sums(two)
    for bit in tp_bits():
        gain_total = gain_total + tp_swap(gain_total, bit)
    gain_shard = fsdp_scatter(gain_total, 1)
    vocab_grad = jnp.stack([table_shard, head_shard])
    attn_grad = jnp.concatenate(
        [self_shards[0:3], cross_shards[0:3], self_shards[3:4], cross_shards[3:4]], axis=0
    )
    ffn_grad = jnp.stack([up_shard, down_shard])
    only_first = (tp_index == 0).astype(f32)
    squares = (
        jnp.sum(vocab_grad * vocab_grad)
        + jnp.sum(attn_grad * attn_grad)
        + jnp.sum(ffn_grad * ffn_grad)
        + only_first * jnp.sum(gain_shard * gain_shard)
    )
    live_local = jnp.sum(clip_weight.astype(f32))
    sums = jnp.stack([squares, (one.numerator + two.numerator) * only_first, live_local * only_first])
    for bit in tp_bits():
        sums = sums + tp_swap(sums, bit)
    for b in range(fsdp_count.bit_length() - 1):
        sums = sums + lax.ppermute(
            sums, "fsdp", [(i, i ^ (1 << b)) for i in range(fsdp_count)]
        )
    per_clip = BOOKS * (frames - 1) - BOOKS * (BOOKS - 1) // 2
    counted_total = sums[2] * per_clip
    step_loss = sums[1] / counted_total
    grad_norm = jnp.sqrt(sums[0])
    factor = jnp.minimum(1.0, clip_scale * jnp.sqrt(counted_total) / (grad_norm + 1e-06))
    step_float = step_count[0].astype(f32)
    vocab_out = adam_update(vocab_tables, vocab_grad, vocab_m, vocab_v, factor, step_float, True)
    attn_out = adam_update(attn_weights, attn_grad, attn_m, attn_v, factor, step_float, True)
    ffn_out = adam_update(ffn_weights, ffn_grad, ffn_m, ffn_v, factor, step_float, True)
    norm_out = adam_update(norm_params, gain_shard, norm_m, norm_v, factor, step_float, False)
    return (step_loss, grad_norm) + vocab_out + attn_out + ffn_out + norm_out


def solution(mesh):
    batch = P(None, "fsdp")
    clip = P(None, "fsdp", None, None)
    table = P(None, None, "fsdp", "tp")
    matrix = P(None, "fsdp", "tp")
    placed = (clip, clip, batch, batch, P(), table, matrix, matrix, batch)
    moments = (table, table, matrix, matrix, matrix, matrix, batch, batch)
    return jax.shard_map(
        per_device,
        mesh=mesh,
        in_specs=placed + moments,
        out_specs=(P(), P()) + (table,) * 4 + (matrix,) * 8 + (batch,) * 4,
        check_vma=False,
    )
```

```python
import functools
import math

import jax
import jax.numpy as jnp
from jax import lax
from jax.experimental import pallas as pl
from jax.experimental.pallas import tpu as pltpu
from jax.sharding import PartitionSpec as P

D = 1024
HEAD_DIM = 64
VOCAB = 2048
BOOKS = 4
MICRO = 2
PAIR = 128

ln_eps = 1e-05
smooth = 0.1
z_weight = 0.01
clip_scale = 24.0
learn_rate = 0.02
beta_one = 0.9
beta_two = 0.95
adam_eps = 1e-08
weight_decay = 0.1
neg_big = -1e30


bf16 = jnp.bfloat16
f16 = jnp.float16
f32 = jnp.float32


def mm(spec, left, right):
    return jnp.einsum(spec, left, right, preferred_element_type=f32)


def fsdp_levels():
    left = lax.axis_size("fsdp")
    levels, stride = [], 1
    for size in (2,) + (4,) * 8:
        size = min(size, left)
        if size == 1:
            break
        levels.append((size, stride))
        stride *= size
        left //= size
    return levels


def digit_of(index, size, stride):
    return index // stride % size


def shifted(index, size, stride, shift):
    digit = digit_of(index, size, stride)
    return index + ((digit + shift) % size - digit) * stride


def fsdp_shift(value, size, stride, shift):
    count = lax.axis_size("fsdp")
    return lax.ppermute(value, "fsdp", [(i, shifted(i, size, stride, shift)) for i in range(count)])


def shifted_all(index, sign):
    found = [index]
    for size, stride in reversed(fsdp_levels()):
        found = [shifted(o, size, stride, sign * s) for s in range(size) for o in found]
    return found


def fsdp_collect(value):
    held = value[None]
    for size, stride in reversed(fsdp_levels()):
        held = jnp.concatenate(
            [held] + [fsdp_shift(held, size, stride, s) for s in range(1, size)], axis=0
        )
    return held


def fsdp_exchange(value, sign):
    levels = fsdp_levels()
    rest = value.shape[1:]
    value = value.reshape(tuple(size for size, _ in levels) + rest)
    for axis, (size, stride) in enumerate(levels):
        parts = [lax.index_in_dim(value, s, axis, False) for s in range(size)]
        parts = parts[:1] + [fsdp_shift(parts[s], size, stride, sign * s) for s in range(1, size)]
        value = jnp.stack(parts, axis=axis)
    return value.reshape((-1,) + rest)


def fsdp_scatter(total, axis, wire):
    index = lax.axis_index("fsdp")
    rows = total.shape[axis] // lax.axis_size("fsdp")
    for size, stride in fsdp_levels():
        shape = total.shape[:axis] + (-1, size, rows) + total.shape[axis + 1 :]
        blocks = total.reshape(shape)
        digit = digit_of(index, size, stride)

        def block(shift):
            taken = lax.dynamic_index_in_dim(blocks, (digit + shift) % size, axis + 1, False)
            return taken.reshape(total.shape[:axis] + (-1,) + total.shape[axis + 1 :])

        held = block(0).astype(f32)
        for s in range(1, size):
            sent = block(-s).astype(wire)
            held = held + fsdp_shift(sent, size, stride, -s).astype(f32)
        total = held
    return total


def tp_swap(value, bit):
    return lax.ppermute(value, "tp", [(i, i ^ bit) for i in range(lax.axis_size("tp"))])


def across():
    return lax.axis_size("tp") // 2


def row_bits():
    return [1 << b for b in range(across().bit_length() - 1)]


def is_high(bit):
    return lax.axis_index("tp") // bit % 2 == 1


def full_rows(held, axis=0):
    for bit in row_bits():
        other = tp_swap(held, bit)
        high = is_high(bit)
        held = jnp.concatenate(
            [jnp.where(high, other, held), jnp.where(high, held, other)], axis=axis
        )
    return held


def row_sums(product, *lefts, axis=-2):
    bits = row_bits()[::-1]
    half = lefts[0].shape[axis] // 2
    high = is_high(bits[0]).astype(jnp.int32)

    def part(side):
        return product(*[lax.dynamic_slice_in_dim(a, side * half, half, axis=axis) for a in lefts])

    sent = part(1 - high)
    total = part(high) + tp_swap(sent, bits[0])
    for bit in bits[1:]:
        half = total.shape[-2] // 2
        high = is_high(bit).astype(jnp.int32)
        sent = lax.dynamic_slice_in_dim(total, (1 - high) * half, half, axis=-2)
        kept = lax.dynamic_slice_in_dim(total, high * half, half, axis=-2)
        total = kept + tp_swap(sent, bit)
    return total


def everywhere(join, value, bits):
    for bit in bits:
        value = join(value, tp_swap(value, bit))
    count = lax.axis_size("fsdp")
    for b in range(count.bit_length() - 1):
        pairs = [(i, i ^ (1 << b)) for i in range(count)]
        value = join(value, lax.ppermute(value, "fsdp", pairs))
    return value


def top_of(value):
    return jnp.max(jnp.abs(value)).astype(f32)


def layer_norm(values, gain_row, shift_row):
    centred = values - jnp.mean(values, axis=-1, keepdims=True)
    spread = jnp.mean(centred * centred, axis=-1, keepdims=True)
    return centred * lax.rsqrt(spread + ln_eps) * gain_row + shift_row


def norm_back(values, gain_row, gradient):
    centred = values - jnp.mean(values, axis=-1, keepdims=True)
    scale = lax.rsqrt(jnp.mean(centred * centred, axis=-1, keepdims=True) + ln_eps)
    normed = centred * scale
    scaled = gradient * gain_row
    step = scale * (
        scaled
        - jnp.mean(scaled, axis=-1, keepdims=True)
        - normed * jnp.mean(scaled * normed, axis=-1, keepdims=True)
    )
    return step, jnp.sum(gradient * normed, axis=0), jnp.sum(gradient, axis=0)


def exact_gelu(values):
    return jax.nn.gelu(values, approximate=False)


def gelu_back(values, gradient):
    _, pullback = jax.vjp(exact_gelu, values)
    return pullback(gradient)[0]


def positions(first_row, row_count, model_width):
    half_width = model_width // 2
    steps = jnp.arange(half_width).astype(f32)
    frequencies = jnp.exp(-math.log(10000.0) * steps / (half_width - 1))
    places = (first_row + jnp.arange(row_count)).astype(f32)
    angles = places[:, None] * frequencies[None, :]
    return jnp.concatenate([jnp.cos(angles), jnp.sin(angles)], axis=1)


def merge_stats(earlier, later):
    row_top = jnp.maximum(earlier[0], later[0])
    row_mass = earlier[1] * jnp.exp(earlier[0] - row_top) + later[1] * jnp.exp(later[0] - row_top)
    return jnp.stack([row_top, row_mass, earlier[2] + later[2], earlier[3] + later[3]])


def contract(left, right, dims):
    return lax.dot_general(left, right, (dims, ((), ())), preferred_element_type=f32)

def spans(tile, step, keys, causal):
    if not causal:
        return [(0, keys, True)]
    start = step * tile
    return ([(0, start, False)] if start else []) + [(start, tile, True)]

def attend_forward_kernel(causal, tile, length_ref, q_ref, k_ref, v_ref, o_ref):
    frames, keys = q_ref.shape[0], k_ref.shape[0]
    scale = HEAD_DIM ** (-0.5)
    lane = lax.broadcasted_iota(jnp.int32, (1, PAIR), 1) // HEAD_DIM
    for step in range(frames // tile):
        queries = q_ref[pl.ds(step * tile, tile), :]
        mixed = None
        for head in range(PAIR // HEAD_DIM):
            own = jnp.where(lane == head, queries, jnp.zeros_like(queries))
            parts = []
            for start, size, masked in spans(tile, step, keys, causal):
                scores = contract(own, k_ref[pl.ds(start, size), :], ((1,), (1,))) * scale
                if masked:
                    column = lax.broadcasted_iota(jnp.int32, scores.shape, 1)
                    if causal:
                        allowed = column <= lax.broadcasted_iota(jnp.int32, scores.shape, 0)
                    else:
                        allowed = column < length_ref[0]
                    scores = jnp.where(allowed, scores, neg_big)
                parts.append(scores)
            top = functools.reduce(jnp.maximum, [jnp.max(p, axis=1, keepdims=True) for p in parts])
            parts = [jnp.exp(p - top) for p in parts]
            mass = sum(jnp.sum(p, axis=1, keepdims=True) for p in parts)
            inverse = 1.0 / mass
            total = None
            for p, (start, size, _) in zip(parts, spans(tile, step, keys, causal)):
                part = contract((p * inverse).astype(bf16), v_ref[pl.ds(start, size), :], ((1,), (0,)))
                total = part if total is None else total + part
            mixed = total if mixed is None else jnp.where(lane == head, total, mixed)
        o_ref[pl.ds(step * tile, tile), :] = mixed.astype(bf16)

def attend_backward_kernel(causal, tile, length_ref, q_ref, k_ref, v_ref, g_ref, dq_ref, dk_ref, dv_ref, dk_acc, dv_acc):
    frames, keys = q_ref.shape[0], k_ref.shape[0]
    scale = HEAD_DIM ** (-0.5)
    lane = lax.broadcasted_iota(jnp.int32, (1, PAIR), 1) // HEAD_DIM
    dk_acc[...] = jnp.zeros_like(dk_acc)
    dv_acc[...] = jnp.zeros_like(dv_acc)
    for step in range(frames // tile):
        queries = q_ref[pl.ds(step * tile, tile), :]
        upstream = g_ref[pl.ds(step * tile, tile), :]
        grad_query = None
        for head in range(PAIR // HEAD_DIM):
            own = jnp.where(lane == head, queries, jnp.zeros_like(queries))
            grad = jnp.where(lane == head, upstream, jnp.zeros_like(upstream))
            ranges = spans(tile, step, keys, causal)
            parts = []
            for start, size, masked in ranges:
                scores = contract(k_ref[pl.ds(start, size), :], own, ((1,), (1,))) * scale
                if masked:
                    row = lax.broadcasted_iota(jnp.int32, scores.shape, 0)
                    if causal:
                        allowed = row <= lax.broadcasted_iota(jnp.int32, scores.shape, 1)
                    else:
                        allowed = row < length_ref[0]
                    scores = jnp.where(allowed, scores, neg_big)
                parts.append(scores)
            top = functools.reduce(jnp.maximum, [jnp.max(p, axis=0, keepdims=True) for p in parts])
            parts = [jnp.exp(p - top) for p in parts]
            inverse = 1.0 / sum(jnp.sum(p, axis=0, keepdims=True) for p in parts)
            parts = [p * inverse for p in parts]
            rises = [contract(v_ref[pl.ds(start, size), :], grad, ((1,), (1,))) for start, size, _ in ranges]
            inner = sum(jnp.sum(p * r, axis=0, keepdims=True) for p, r in zip(parts, rises))
            for p, r, (start, size, _) in zip(parts, rises, ranges):
                where = pl.ds(start, size)
                dv_acc[where, :] += contract(p.astype(bf16), grad, ((1,), (0,)))
                slope = (p * (r - inner)).astype(bf16)
                dk_acc[where, :] += contract(slope, own, ((1,), (0,)))
                near = k_ref[where, :]
                near = jnp.where(lane == head, near, jnp.zeros_like(near))
                part = contract(slope, near, ((0,), (0,)))
                grad_query = part if grad_query is None else grad_query + part
        dq_ref[pl.ds(step * tile, tile), :] = (grad_query * scale).astype(bf16)
    dk_ref[...] = (dk_acc[...] * scale).astype(bf16)
    dv_ref[...] = dv_acc[...].astype(bf16)


def pair_spec(rows, first):
    return pl.BlockSpec((rows, PAIR), lambda i, length: (0, first + i))


def attend_forward(sources, firsts, cols, length, causal):
    rows, keys = sources[0].shape[0], sources[1].shape[0]
    tile = rows // 2 if causal else rows
    return pl.pallas_call(
        functools.partial(attend_forward_kernel, causal, tile),
        out_shape=jax.ShapeDtypeStruct((rows, cols), bf16),
        grid_spec=pltpu.PrefetchScalarGridSpec(
            num_scalar_prefetch=1,
            grid=(cols // PAIR,),
            in_specs=[pair_spec(s.shape[0], f // PAIR) for s, f in zip(sources, firsts)],
            out_specs=pair_spec(rows, 0),
        ),
        cost_estimate=pl.CostEstimate(
            flops=20 * rows * keys * cols,
            bytes_accessed=8 * rows * cols,
            transcendentals=rows * keys * cols // HEAD_DIM,
        ),
    )(length, *sources)


def attend_backward(sources, firsts, cols, length, causal):
    rows, keys = sources[0].shape[0], sources[1].shape[0]
    tile = rows // 2 if causal else rows
    return pl.pallas_call(
        functools.partial(attend_backward_kernel, causal, tile),
        out_shape=[jax.ShapeDtypeStruct((s.shape[0], cols), bf16) for s in sources[:3]],
        grid_spec=pltpu.PrefetchScalarGridSpec(
            num_scalar_prefetch=1,
            grid=(cols // PAIR,),
            in_specs=[pair_spec(s.shape[0], f // PAIR) for s, f in zip(sources, firsts)],
            out_specs=[pair_spec(s.shape[0], 0) for s in sources[:3]],
            scratch_shapes=[pltpu.VMEM((keys, PAIR), f32)] * 2,
        ),
        cost_estimate=pl.CostEstimate(
            flops=40 * rows * keys * cols,
            bytes_accessed=16 * rows * cols,
            transcendentals=rows * keys * cols // HEAD_DIM,
        ),
    )(length, *sources)


def adam_update(master, gradient, moment_one, moment_two, factor, step_float, decayed):
    clipped = gradient * factor
    moment_one = beta_one * moment_one + (1.0 - beta_one) * clipped
    moment_two = beta_two * moment_two + (1.0 - beta_two) * clipped * clipped
    fix_one = 1.0 - jnp.power(beta_one, step_float)
    fix_two = 1.0 - jnp.power(beta_two, step_float)
    change = moment_one / fix_one / (jnp.sqrt(moment_two / fix_two) + adam_eps)
    if decayed:
        change = change + weight_decay * master
    updated = master - learn_rate * change
    return (updated, moment_one, moment_two, updated.astype(bf16))


def per_device(
    audio_codes,
    text_states,
    clip_weight,
    text_length,
    step_count,
    vocab_tables,
    attn_weights,
    ffn_weights,
    norm_params,
    vocab_m,
    vocab_v,
    attn_m,
    attn_v,
    ffn_m,
    ffn_v,
    norm_m,
    norm_v,
):
    tp_index = lax.axis_index("tp")
    fsdp_index = lax.axis_index("fsdp")
    fsdp_count = lax.axis_size("fsdp")
    far = across()
    clip = tp_index // far
    frames = audio_codes.shape[3]
    local_rows = frames // far
    first_row = tp_index % far * local_rows
    shard_rows = D // fsdp_count
    vocab_local = vocab_tables.shape[3]
    cols = attn_weights.shape[2]
    halves = (0, 1)

    def of_clip(values):
        return lax.dynamic_index_in_dim(values[:, 0], clip, 0, False)

    table_low = vocab_tables.astype(bf16)
    attn_low = attn_weights.astype(bf16)
    ffn_low = ffn_weights.astype(bf16)
    norm_low = jnp.pad(norm_params.astype(bf16).T, ((0, 0), (0, cols - 8)))
    embed_tables = jnp.concatenate([table_low[0], tp_swap(table_low[0], far)], axis=2)
    self_own = jnp.concatenate([attn_low[j] for j in (0, 1, 2, 6)], axis=1)
    self_far = tp_swap(self_own, far)
    wide = 3 * cols
    self_shard = jnp.stack(
        [
            self_own[:, :wide],
            self_far[:, :wide],
            jnp.concatenate([self_own[:, wide:], self_far[:, wide:], norm_low], axis=1),
        ]
    )
    self_full = lax.all_gather(self_shard, "fsdp", axis=1, tiled=True)
    in_self = (self_full[0], self_full[1])
    out_self = (self_full[2, :, :cols], self_full[2, :, cols : 2 * cols])
    gains = self_full[2, :, 2 * cols : 2 * cols + 8].T.astype(f32)
    cross_shard = jnp.stack([attn_low[j] for j in (3, 4, 5, 7)])
    cross_own = lax.all_gather(cross_shard, "fsdp", axis=1, tiled=True)
    cross_far = tp_swap(cross_own, far)
    in_query = (cross_own[0], cross_far[0])
    in_text = (cross_own[1:3], cross_far[1:3])
    out_cross = (cross_own[3], cross_far[3])
    ffn_own = lax.all_gather(ffn_low, "fsdp", axis=1, tiled=True)
    up = (ffn_own[0], tp_swap(ffn_own[0], far))
    down = (ffn_own[1], tp_swap(ffn_own[1], far))
    head_shard = jnp.concatenate([table_low[1], tp_swap(table_low[1], far)], axis=0)
    head_full = lax.all_gather(head_shard, "fsdp", axis=1, tiled=True)
    heads = (head_full[:BOOKS], head_full[BOOKS:])

    frame_ids = jnp.arange(frames)
    book_ids = jnp.arange(BOOKS)[:, None]
    live_mask = frame_ids[None, :] >= book_ids
    counted = (live_mask & (frame_ids[None, :] <= frames - 2)).astype(f32)
    own_ids = jnp.arange(vocab_local)
    half_ids = (tp_index * vocab_local + own_ids, (tp_index ^ far) * vocab_local + own_ids)
    table_ids = jnp.concatenate(half_ids)

    codes = of_clip(audio_codes)
    text = of_clip(text_states)
    live = lax.dynamic_index_in_dim(clip_weight[:, 0], clip, 0, False).astype(f32)
    length = lax.dynamic_slice_in_dim(text_length[:, 0], clip, 1)

    live_codes = fsdp_collect(jnp.where(live_mask, codes, -1))

    def chosen_entries(ids):
        return (ids[..., None] == table_ids).astype(bf16)

    embedded = row_sums(
        lambda ids: mm("ckfv,kdv->cfd", chosen_entries(ids), embed_tables), live_codes, axis=-1
    )
    pieces = fsdp_exchange(embedded, -1)

    def place_of(block):
        place = 0
        for size, stride in fsdp_levels():
            gap = digit_of(block, size, stride) - digit_of(fsdp_index, size, stride)
            place = place * size + gap % size
        return place

    state_zero = jnp.concatenate(
        [lax.dynamic_index_in_dim(pieces, place_of(b), 0, False) for b in range(fsdp_count)], axis=1
    ) + positions(first_row, local_rows, D)

    rows_one = full_rows(layer_norm(state_zero, gains[0], gains[4]).astype(bf16))
    self_proj = [mm("fd,de->fe", rows_one, in_self[h]).astype(bf16) for h in halves]
    self_from = (0, cols, 2 * cols)
    mixed_one = [attend_forward((p, p, p), self_from, cols, length, True) for p in self_proj]

    def project(left, right):
        return mm("fe,de->fd", left, right)

    def project_out(weights):
        return lambda a, b: project(a, weights[0]) + project(b, weights[1])

    state_one = state_zero + row_sums(project_out(out_self), *mixed_one)
    rows_two = full_rows(layer_norm(state_one, gains[1], gains[5]).astype(bf16))
    cross_query = [mm("fd,de->fe", rows_two, in_query[h]).astype(bf16) for h in halves]
    cross_kv = [mm("td,jde->jte", text, in_text[h]).astype(bf16) for h in halves]
    mixed_two = [
        attend_forward((q, kv[0], kv[1]), (0, 0, 0), cols, length, False)
        for q, kv in zip(cross_query, cross_kv)
    ]
    state_two = state_one + row_sums(project_out(out_cross), *mixed_two)
    rows_three = full_rows(layer_norm(state_two, gains[2], gains[6]).astype(bf16))
    hidden_pre = [mm("fd,de->fe", rows_three, up[h]) for h in halves]
    active = [exact_gelu(a).astype(bf16) for a in hidden_pre]
    state_three = state_two + row_sums(project_out(down), *active)
    rows_four = full_rows(layer_norm(state_three, gains[3], gains[7]).astype(bf16))
    targets = jnp.concatenate([codes[:, 1:], jnp.zeros((BOOKS, 1), jnp.int32)], axis=1)
    logits = [mm("fd,kdv->kfv", rows_four, heads[h]) for h in halves]
    chosen = [targets[..., None] == half_ids[h] for h in halves]

    def half_stats(z, hit):
        top = jnp.max(z, axis=-1)
        mass = jnp.sum(jnp.exp(z - top[..., None]), axis=-1)
        picked = jnp.sum(jnp.where(hit, z, 0.0), axis=-1)
        return jnp.stack([top, mass, picked, jnp.sum(z, axis=-1)])

    stats = merge_stats(half_stats(logits[0], chosen[0]), half_stats(logits[1], chosen[1]))
    for bit in row_bits():
        stats = merge_stats(stats, tp_swap(stats, bit))
    log_total = stats[0] + jnp.log(stats[1])
    loss_terms = (
        log_total
        - (1.0 - smooth) * stats[2]
        - smooth * stats[3] / VOCAB
        + z_weight * log_total * log_total
    )
    numerator = live * jnp.sum(loss_terms * counted)
    row_scale = (live * counted)[..., None]

    def logit_gradient(z, hit):
        prob_rows = jnp.exp(z - log_total[..., None])
        return (
            row_scale
            * (
                prob_rows * (1.0 + 2.0 * z_weight * log_total[..., None])
                - (1.0 - smooth) * hit.astype(f32)
                - smooth / VOCAB
            )
        ).astype(bf16)

    grad_logits = [logit_gradient(logits[h], chosen[h]) for h in halves]

    total_rows = float(frames * MICRO * fsdp_count)

    def wire_scale(*bounds):
        bound = functools.reduce(jnp.maximum, bounds) * total_rows
        return 32768.0 / jnp.maximum(everywhere(jnp.maximum, bound, (far,)), 1e-30)

    def scatter(scale, pair):
        own, other = [(g * scale).astype(f16) for g in pair]
        joined = (own.astype(f32) + tp_swap(other, far).astype(f32)).astype(f16)
        return fsdp_scatter(joined, joined.ndim - 2, f16) / scale

    def project_back(left, right):
        return mm("fd,de->fe", left, right)

    def weight_grad(left, right):
        return mm("fd,fe->de", left, right)

    grad_rows = row_sums(
        lambda a, b: mm("kfv,kdv->fd", a, heads[0]) + mm("kfv,kdv->fd", b, heads[1]), *grad_logits
    )
    head_scale = wire_scale(top_of(rows_four) * jnp.maximum(*[top_of(g) for g in grad_logits]))
    head_grad = scatter(head_scale, [mm("kfv,fd->kdv", g, rows_four) for g in grad_logits])
    grad_state, gain_four, shift_four = norm_back(state_three, gains[3], grad_rows)

    grad_out = full_rows(grad_state.astype(bf16))
    grad_hidden = [
        gelu_back(hidden_pre[h], project_back(grad_out, down[h])).astype(bf16) for h in halves
    ]
    step, gain_three, shift_three = norm_back(
        state_two, gains[2], row_sums(project_out(up), *grad_hidden)
    )
    ffn_scale = wire_scale(
        top_of(rows_three) * jnp.maximum(*[top_of(g) for g in grad_hidden]),
        top_of(grad_out) * jnp.maximum(*[top_of(u) for u in active]),
    )
    up_grad = scatter(ffn_scale, [weight_grad(rows_three, grad_hidden[h]) for h in halves])
    down_grad = scatter(ffn_scale, [weight_grad(grad_out, active[h]) for h in halves])
    grad_state = grad_state + step

    grad_out = full_rows(grad_state.astype(bf16))
    grad_mixed = [project_back(grad_out, out_cross[h]).astype(bf16) for h in halves]
    grad_cross = [
        attend_backward((q, kv[0], kv[1], g), (0, 0, 0, 0), cols, length, False)
        for q, kv, g in zip(cross_query, cross_kv, grad_mixed)
    ]
    step, gain_two, shift_two = norm_back(
        state_one, gains[1], row_sums(project_out(in_query), *[g[0] for g in grad_cross])
    )
    cross_scale = wire_scale(
        top_of(rows_two) * jnp.maximum(*[top_of(g[0]) for g in grad_cross]),
        top_of(text) * functools.reduce(jnp.maximum, [top_of(k) for g in grad_cross for k in g[1:]]),
        top_of(grad_out) * jnp.maximum(*[top_of(o) for o in mixed_two]),
    )
    cross_grad = scatter(
        cross_scale,
        [
            jnp.concatenate(
                [
                    weight_grad(rows_two, grad_cross[h][0]),
                    weight_grad(text, grad_cross[h][1]),
                    weight_grad(text, grad_cross[h][2]),
                    weight_grad(grad_out, mixed_two[h]),
                ],
                axis=1,
            )
            for h in halves
        ],
    )
    grad_state = grad_state + step

    grad_out = full_rows(grad_state.astype(bf16))
    grad_mixed = [project_back(grad_out, out_self[h]).astype(bf16) for h in halves]
    grad_self = [
        jnp.concatenate(attend_backward((p, p, p, g), self_from + (0,), cols, length, True), axis=1)
        for p, g in zip(self_proj, grad_mixed)
    ]
    step, gain_one, shift_one = norm_back(
        state_zero, gains[0], row_sums(project_out(in_self), *grad_self)
    )
    self_scale = wire_scale(
        top_of(rows_one) * jnp.maximum(*[top_of(g) for g in grad_self]),
        top_of(grad_out) * jnp.maximum(*[top_of(o) for o in mixed_one]),
    )
    self_grad = scatter(
        self_scale,
        [
            jnp.concatenate(
                [weight_grad(rows_one, grad_self[h]), weight_grad(grad_out, mixed_one[h])], axis=1
            )
            for h in halves
        ],
    )
    grad_embed = (grad_state + step).astype(bf16)
    sent_blocks = jnp.stack(
        [
            lax.dynamic_slice_in_dim(grad_embed, o * shard_rows, shard_rows, axis=1)
            for o in shifted_all(fsdp_index, 1)
        ]
    )
    embed_rows = full_rows(fsdp_exchange(sent_blocks, 1), axis=1)
    table_parts = mm("ckfv,cfd->kdv", chosen_entries(live_codes), embed_rows)
    table_grad = table_parts[..., :vocab_local] + tp_swap(table_parts[..., vocab_local:], far)

    gain_total = jnp.stack(
        [gain_one, gain_two, gain_three, gain_four, shift_one, shift_two, shift_three, shift_four]
    )
    for bit in row_bits() + [far]:
        gain_total = gain_total + tp_swap(gain_total, bit)
    gain_grad = fsdp_scatter(gain_total[..., None], 1, f32)[..., 0]

    vocab_grad = jnp.stack([table_grad, head_grad])
    self_parts = jnp.split(self_grad, 4, axis=1)
    cross_parts = jnp.split(cross_grad, 4, axis=1)
    attn_grad = jnp.stack(
        self_parts[:3] + cross_parts[:3] + [self_parts[3], cross_parts[3]], axis=0
    )
    ffn_grad = jnp.stack([up_grad, down_grad])
    only_first = (tp_index == 0).astype(f32)
    squares = (
        jnp.sum(vocab_grad * vocab_grad)
        + jnp.sum(attn_grad * attn_grad)
        + jnp.sum(ffn_grad * ffn_grad)
        + only_first * jnp.sum(gain_grad * gain_grad)
    )
    once = (tp_index % far == 0).astype(f32)
    sums = jnp.stack([squares, numerator * once, live * once])
    sums = everywhere(jnp.add, sums, row_bits() + [far])
    per_clip = BOOKS * (frames - 1) - BOOKS * (BOOKS - 1) // 2
    counted_total = sums[2] * per_clip
    step_loss = sums[1] / counted_total
    grad_norm = jnp.sqrt(sums[0])
    factor = jnp.minimum(1.0, clip_scale * jnp.sqrt(counted_total) / (grad_norm + 1e-06))
    step_float = step_count[0].astype(f32)
    vocab_out = adam_update(vocab_tables, vocab_grad, vocab_m, vocab_v, factor, step_float, True)
    attn_out = adam_update(attn_weights, attn_grad, attn_m, attn_v, factor, step_float, True)
    ffn_out = adam_update(ffn_weights, ffn_grad, ffn_m, ffn_v, factor, step_float, True)
    norm_out = adam_update(norm_params, gain_grad, norm_m, norm_v, factor, step_float, False)
    return (step_loss, grad_norm) + vocab_out + attn_out + ffn_out + norm_out


def solution(mesh):
    batch = P(None, "fsdp")
    clip = P(None, "fsdp", None, None)
    table = P(None, None, "fsdp", "tp")
    matrix = P(None, "fsdp", "tp")
    placed = (clip, clip, batch, batch, P(), table, matrix, matrix, batch)
    moments = (table, table, matrix, matrix, matrix, matrix, batch, batch)
    return jax.shard_map(
        per_device,
        mesh=mesh,
        in_specs=placed + moments,
        out_specs=(P(), P()) + (table,) * 4 + (matrix,) * 8 + (batch,) * 4,
        check_vma=False,
    )
```

```python
import functools
import math

import jax
import jax.numpy as jnp
from jax import lax
from jax.experimental import pallas as pl
from jax.experimental.pallas import tpu as pltpu
from jax.sharding import PartitionSpec as P

D = 1024
HEAD_DIM = 64
VOCAB = 2048
BOOKS = 4
MICRO = 2
PAIR = 128

ln_eps = 1e-05
smooth = 0.1
z_weight = 0.01
clip_scale = 24.0
learn_rate = 0.02
beta_one = 0.9
beta_two = 0.95
adam_eps = 1e-08
weight_decay = 0.1
neg_big = -1e30


bf16 = jnp.bfloat16
f16 = jnp.float16
f32 = jnp.float32


def mm(spec, left, right):
    return jnp.einsum(spec, left, right, preferred_element_type=f32)


def fsdp_levels():
    left = lax.axis_size("fsdp")
    levels, stride = [], 1
    for size in (2,) + (4,) * 8:
        size = min(size, left)
        if size == 1:
            break
        levels.append((size, stride))
        stride *= size
        left //= size
    return levels


def digit_of(index, size, stride):
    return index // stride % size


def shifted(index, size, stride, shift):
    digit = digit_of(index, size, stride)
    return index + ((digit + shift) % size - digit) * stride


def fsdp_shift(value, size, stride, shift):
    count = lax.axis_size("fsdp")
    return lax.ppermute(value, "fsdp", [(i, shifted(i, size, stride, shift)) for i in range(count)])


def shifted_all(index, sign):
    found = [index]
    for size, stride in reversed(fsdp_levels()):
        found = [shifted(o, size, stride, sign * s) for s in range(size) for o in found]
    return found


def fsdp_collect(value):
    held = value[None]
    for size, stride in reversed(fsdp_levels()):
        held = jnp.concatenate(
            [held] + [fsdp_shift(held, size, stride, s) for s in range(1, size)], axis=0
        )
    return held


def fsdp_exchange(value, sign, tie=None):
    levels = fsdp_levels()
    rest = value.shape[1:]
    value = value.reshape(tuple(size for size, _ in levels) + rest)
    for axis, (size, stride) in enumerate(levels):
        parts = [lax.index_in_dim(value, s, axis, False) for s in range(size)]
        if axis and tie is not None:
            parts = [p + tie for p in parts]
        parts = parts[:1] + [fsdp_shift(parts[s], size, stride, sign * s) for s in range(1, size)]
        value = jnp.stack(parts, axis=axis)
    return value.reshape((-1,) + rest)


def zero_of(value):
    return value.reshape(-1)[0].astype(f32) * 0.0


def tp_swap(value, bit):
    return lax.ppermute(value, "tp", [(i, i ^ bit) for i in range(lax.axis_size("tp"))])


def digit_block(value, axis, level, shift):
    size, stride = level
    rows = value.shape[axis]
    for other, _ in fsdp_levels()[fsdp_levels().index(level) :]:
        rows //= other
    axis %= value.ndim
    blocks = value.reshape(value.shape[:axis] + (-1, size, rows) + value.shape[axis + 1 :])
    digit = (digit_of(lax.axis_index("fsdp"), size, stride) + shift) % size
    taken = lax.dynamic_index_in_dim(blocks, digit, axis + 1, False)
    return taken.reshape(value.shape[:axis] + (-1,) + value.shape[axis + 1 :])


def sum_of(parts):
    return sum(p.astype(f32) for p in parts)


def level_hop(parts, level, wire, tie=0.0):
    size, stride = level
    came = []
    for s in range(1, size):
        sent = (sum_of([digit_block(p, -2, level, -s) for p in parts]) + tie).astype(wire)
        came.append(fsdp_shift(sent, size, stride, -s))
    return [digit_block(p, -2, level, 0) for p in parts] + came


def swapped(value):
    return tp_swap(value, across())


def across_first(left, product, wire):
    parts = [product(left, 0).astype(wire), swapped(product(left, 1).astype(wire))]
    for level in fsdp_levels():
        tie = yield
        parts = level_hop(parts, level, wire, tie)
    tie = yield
    yield sum_of(parts) + tie


def across_last(left, product, wire):
    first = fsdp_levels()[0]
    size, stride = first
    sets = []
    picks = [[digit_block(a, -1, first, -s) for a in left] for s in range(size)]
    for h in (1, 0):
        came = [
            fsdp_shift(product(picks[s], h).astype(wire), size, stride, -s) for s in range(1, size)
        ]
        sets.append([product(picks[0], h).astype(wire)] + came)
    for level in fsdp_levels()[1:]:
        tie = yield
        sets = [level_hop(parts, level, wire, tie) for parts in sets]
    tie = yield
    came = swapped((sum_of(sets[0]) + tie).astype(wire))
    tie = yield
    yield sum_of(sets[1] + [came]) + tie


def finish(hops, anchor=0.0):
    result = None
    while result is None:
        result = hops.send(anchor)
    return result


def fsdp_scatter(total):
    parts = [total]
    for level in fsdp_levels():
        parts = level_hop(parts, level, f32)
    return sum_of(parts)


def across():
    return lax.axis_size("tp") // 2


def row_bits():
    return [1 << b for b in range(across().bit_length() - 1)]


def is_high(bit):
    return lax.axis_index("tp") // bit % 2 == 1


def full_rows(held, axis=0):
    for bit in row_bits():
        other = tp_swap(held, bit)
        high = is_high(bit)
        held = jnp.concatenate(
            [jnp.where(high, other, held), jnp.where(high, held, other)], axis=axis
        )
    return held


def row_sums(product, *lefts, axis=-2):
    bits = row_bits()[::-1]
    half = lefts[0].shape[axis] // 2
    high = is_high(bits[0]).astype(jnp.int32)

    def part(side):
        return product(*[lax.dynamic_slice_in_dim(a, side * half, half, axis=axis) for a in lefts])

    sent = part(1 - high)
    total = part(high) + tp_swap(sent, bits[0])
    for bit in bits[1:]:
        half = total.shape[-2] // 2
        high = is_high(bit).astype(jnp.int32)
        sent = lax.dynamic_slice_in_dim(total, (1 - high) * half, half, axis=-2)
        kept = lax.dynamic_slice_in_dim(total, high * half, half, axis=-2)
        total = kept + tp_swap(sent, bit)
    return total


def everywhere(join, value, bits):
    for bit in bits:
        value = join(value, tp_swap(value, bit))
    count = lax.axis_size("fsdp")
    for b in range(count.bit_length() - 1):
        pairs = [(i, i ^ (1 << b)) for i in range(count)]
        value = join(value, lax.ppermute(value, "fsdp", pairs))
    return value


def layer_norm(values, gain_row, shift_row):
    centred = values - jnp.mean(values, axis=-1, keepdims=True)
    spread = jnp.mean(centred * centred, axis=-1, keepdims=True)
    return centred * lax.rsqrt(spread + ln_eps) * gain_row + shift_row


def norm_back(values, gain_row, gradient):
    centred = values - jnp.mean(values, axis=-1, keepdims=True)
    scale = lax.rsqrt(jnp.mean(centred * centred, axis=-1, keepdims=True) + ln_eps)
    normed = centred * scale
    scaled = gradient * gain_row
    step = scale * (
        scaled
        - jnp.mean(scaled, axis=-1, keepdims=True)
        - normed * jnp.mean(scaled * normed, axis=-1, keepdims=True)
    )
    return step, jnp.sum(gradient * normed, axis=0), jnp.sum(gradient, axis=0)


def exact_gelu(values):
    return jax.nn.gelu(values, approximate=False)


def gelu_back(values, gradient):
    _, pullback = jax.vjp(exact_gelu, values)
    return pullback(gradient)[0]


def positions(first_row, row_count, model_width):
    half_width = model_width // 2
    steps = jnp.arange(half_width).astype(f32)
    frequencies = jnp.exp(-math.log(10000.0) * steps / (half_width - 1))
    places = (first_row + jnp.arange(row_count)).astype(f32)
    angles = places[:, None] * frequencies[None, :]
    return jnp.concatenate([jnp.cos(angles), jnp.sin(angles)], axis=1)


def merge_stats(earlier, later):
    row_top = jnp.maximum(earlier[0], later[0])
    row_mass = earlier[1] * jnp.exp(earlier[0] - row_top) + later[1] * jnp.exp(later[0] - row_top)
    return jnp.stack([row_top, row_mass, earlier[2] + later[2], earlier[3] + later[3]])


def contract(left, right, dims):
    return lax.dot_general(left, right, (dims, ((), ())), preferred_element_type=f32)

def spans(tile, step, keys, causal):
    if not causal:
        return [(0, keys, True)]
    start = step * tile
    return ([(0, start, False)] if start else []) + [(start, tile, True)]

def attend_forward_kernel(causal, tile, length_ref, q_ref, k_ref, v_ref, o_ref):
    frames, keys = q_ref.shape[0], k_ref.shape[0]
    scale = HEAD_DIM ** (-0.5)
    lane = lax.broadcasted_iota(jnp.int32, (1, PAIR), 1) // HEAD_DIM
    for step in range(frames // tile):
        queries = q_ref[pl.ds(step * tile, tile), :]
        mixed = None
        for head in range(PAIR // HEAD_DIM):
            own = jnp.where(lane == head, queries, jnp.zeros_like(queries))
            parts = []
            for start, size, masked in spans(tile, step, keys, causal):
                scores = contract(own, k_ref[pl.ds(start, size), :], ((1,), (1,))) * scale
                if masked:
                    column = lax.broadcasted_iota(jnp.int32, scores.shape, 1)
                    if causal:
                        allowed = column <= lax.broadcasted_iota(jnp.int32, scores.shape, 0)
                    else:
                        allowed = column < length_ref[0]
                    scores = jnp.where(allowed, scores, neg_big)
                parts.append(scores)
            top = functools.reduce(jnp.maximum, [jnp.max(p, axis=1, keepdims=True) for p in parts])
            parts = [jnp.exp(p - top) for p in parts]
            mass = sum(jnp.sum(p, axis=1, keepdims=True) for p in parts)
            inverse = 1.0 / mass
            total = None
            for p, (start, size, _) in zip(parts, spans(tile, step, keys, causal)):
                part = contract((p * inverse).astype(bf16), v_ref[pl.ds(start, size), :], ((1,), (0,)))
                total = part if total is None else total + part
            mixed = total if mixed is None else jnp.where(lane == head, total, mixed)
        o_ref[pl.ds(step * tile, tile), :] = mixed.astype(bf16)

def attend_backward_kernel(causal, tile, length_ref, q_ref, k_ref, v_ref, g_ref, dq_ref, dk_ref, dv_ref, dk_acc, dv_acc):
    frames, keys = q_ref.shape[0], k_ref.shape[0]
    scale = HEAD_DIM ** (-0.5)
    lane = lax.broadcasted_iota(jnp.int32, (1, PAIR), 1) // HEAD_DIM
    dk_acc[...] = jnp.zeros_like(dk_acc)
    dv_acc[...] = jnp.zeros_like(dv_acc)
    for step in range(frames // tile):
        queries = q_ref[pl.ds(step * tile, tile), :]
        upstream = g_ref[pl.ds(step * tile, tile), :]
        grad_query = None
        for head in range(PAIR // HEAD_DIM):
            own = jnp.where(lane == head, queries, jnp.zeros_like(queries))
            grad = jnp.where(lane == head, upstream, jnp.zeros_like(upstream))
            ranges = spans(tile, step, keys, causal)
            parts = []
            for start, size, masked in ranges:
                scores = contract(k_ref[pl.ds(start, size), :], own, ((1,), (1,))) * scale
                if masked:
                    row = lax.broadcasted_iota(jnp.int32, scores.shape, 0)
                    if causal:
                        allowed = row <= lax.broadcasted_iota(jnp.int32, scores.shape, 1)
                    else:
                        allowed = row < length_ref[0]
                    scores = jnp.where(allowed, scores, neg_big)
                parts.append(scores)
            top = functools.reduce(jnp.maximum, [jnp.max(p, axis=0, keepdims=True) for p in parts])
            parts = [jnp.exp(p - top) for p in parts]
            inverse = 1.0 / sum(jnp.sum(p, axis=0, keepdims=True) for p in parts)
            parts = [p * inverse for p in parts]
            rises = [contract(v_ref[pl.ds(start, size), :], grad, ((1,), (1,))) for start, size, _ in ranges]
            inner = sum(jnp.sum(p * r, axis=0, keepdims=True) for p, r in zip(parts, rises))
            for p, r, (start, size, _) in zip(parts, rises, ranges):
                where = pl.ds(start, size)
                dv_acc[where, :] += contract(p.astype(bf16), grad, ((1,), (0,)))
                slope = (p * (r - inner)).astype(bf16)
                dk_acc[where, :] += contract(slope, own, ((1,), (0,)))
                near = k_ref[where, :]
                near = jnp.where(lane == head, near, jnp.zeros_like(near))
                part = contract(slope, near, ((0,), (0,)))
                grad_query = part if grad_query is None else grad_query + part
        dq_ref[pl.ds(step * tile, tile), :] = (grad_query * scale).astype(bf16)
    dk_ref[...] = (dk_acc[...] * scale).astype(bf16)
    dv_ref[...] = dv_acc[...].astype(bf16)


def pair_spec(rows, first):
    return pl.BlockSpec((rows, PAIR), lambda i, length: (0, first + i))


def attend_forward(sources, firsts, cols, length, causal):
    rows, keys = sources[0].shape[0], sources[1].shape[0]
    tile = rows // 2 if causal else rows
    return pl.pallas_call(
        functools.partial(attend_forward_kernel, causal, tile),
        out_shape=jax.ShapeDtypeStruct((rows, cols), bf16),
        grid_spec=pltpu.PrefetchScalarGridSpec(
            num_scalar_prefetch=1,
            grid=(cols // PAIR,),
            in_specs=[pair_spec(s.shape[0], f // PAIR) for s, f in zip(sources, firsts)],
            out_specs=pair_spec(rows, 0),
        ),
        cost_estimate=pl.CostEstimate(
            flops=20 * rows * keys * cols,
            bytes_accessed=8 * rows * cols,
            transcendentals=rows * keys * cols // HEAD_DIM,
        ),
    )(length, *sources)


def attend_backward(sources, firsts, cols, length, causal):
    rows, keys = sources[0].shape[0], sources[1].shape[0]
    tile = rows // 2 if causal else rows
    return pl.pallas_call(
        functools.partial(attend_backward_kernel, causal, tile),
        out_shape=[jax.ShapeDtypeStruct((s.shape[0], cols), bf16) for s in sources[:3]],
        grid_spec=pltpu.PrefetchScalarGridSpec(
            num_scalar_prefetch=1,
            grid=(cols // PAIR,),
            in_specs=[pair_spec(s.shape[0], f // PAIR) for s, f in zip(sources, firsts)],
            out_specs=[pair_spec(s.shape[0], 0) for s in sources[:3]],
            scratch_shapes=[pltpu.VMEM((keys, PAIR), f32)] * 2,
        ),
        cost_estimate=pl.CostEstimate(
            flops=40 * rows * keys * cols,
            bytes_accessed=16 * rows * cols,
            transcendentals=rows * keys * cols // HEAD_DIM,
        ),
    )(length, *sources)


def adam_update(master, gradient, moment_one, moment_two, factor, step_float, decayed):
    clipped = gradient * factor
    moment_one = beta_one * moment_one + (1.0 - beta_one) * clipped
    moment_two = beta_two * moment_two + (1.0 - beta_two) * clipped * clipped
    fix_one = 1.0 - jnp.power(beta_one, step_float)
    fix_two = 1.0 - jnp.power(beta_two, step_float)
    change = moment_one / fix_one / (jnp.sqrt(moment_two / fix_two) + adam_eps)
    if decayed:
        change = change + weight_decay * master
    updated = master - learn_rate * change
    return (updated, moment_one, moment_two, updated.astype(bf16))


def per_device(
    audio_codes,
    text_states,
    clip_weight,
    text_length,
    step_count,
    vocab_tables,
    attn_weights,
    ffn_weights,
    norm_params,
    vocab_m,
    vocab_v,
    attn_m,
    attn_v,
    ffn_m,
    ffn_v,
    norm_m,
    norm_v,
):
    tp_index = lax.axis_index("tp")
    fsdp_index = lax.axis_index("fsdp")
    fsdp_count = lax.axis_size("fsdp")
    far = across()
    clip = tp_index // far
    frames = audio_codes.shape[3]
    local_rows = frames // far
    first_row = tp_index % far * local_rows
    shard_rows = D // fsdp_count
    vocab_local = vocab_tables.shape[3]
    cols = attn_weights.shape[2]
    halves = (0, 1)

    def of_clip(values):
        return lax.dynamic_index_in_dim(values[:, 0], clip, 0, False)

    table_low = vocab_tables.astype(bf16)
    attn_low = attn_weights.astype(bf16)
    ffn_low = ffn_weights.astype(bf16)
    norm_low = jnp.pad(norm_params.astype(bf16).T, ((0, 0), (0, cols - 8)))
    embed_tables = jnp.concatenate([table_low[0], tp_swap(table_low[0], far)], axis=2)
    def side_by_side(*picks):
        return jnp.concatenate([attn_low[j] for j in picks], axis=1)

    attn_shard = jnp.stack(
        [
            side_by_side(0, 1, 2),
            jnp.concatenate([side_by_side(6, 7), norm_low], axis=1),
            side_by_side(3, 4, 5),
        ]
    )
    attn_own = lax.all_gather(attn_shard, "fsdp", axis=1, tiled=True)
    attn_ready = zero_of(attn_own)
    in_self = (attn_own[0], swapped(attn_own[0]))
    outs = (attn_own[1, :, : 2 * cols], swapped(attn_own[1, :, : 2 * cols]))
    out_self = [o[:, :cols] for o in outs]
    out_cross = [o[:, cols:] for o in outs]
    gains = attn_own[1, :, 2 * cols : 2 * cols + 8].T.astype(f32)
    in_cross = (attn_own[2], swapped(attn_own[2]))
    in_query = [w[:, :cols] for w in in_cross]
    in_text = [w[:, cols:] for w in in_cross]
    ffn_own = lax.all_gather((ffn_low + attn_ready).astype(bf16), "fsdp", axis=1, tiled=True)
    ffn_ready = zero_of(ffn_own)
    up = (ffn_own[0], swapped(ffn_own[0]))
    down = (ffn_own[1], swapped(ffn_own[1]))
    head_shard = jnp.concatenate([table_low[1], swapped(table_low[1])], axis=0)
    head_full = lax.all_gather((head_shard + ffn_ready).astype(bf16), "fsdp", axis=1, tiled=True)
    heads = (head_full[:BOOKS], head_full[BOOKS:])

    frame_ids = jnp.arange(frames)
    book_ids = jnp.arange(BOOKS)[:, None]
    live_mask = frame_ids[None, :] >= book_ids
    counted = (live_mask & (frame_ids[None, :] <= frames - 2)).astype(f32)
    own_ids = jnp.arange(vocab_local)
    half_ids = (tp_index * vocab_local + own_ids, (tp_index ^ far) * vocab_local + own_ids)
    table_ids = jnp.concatenate(half_ids)

    codes = of_clip(audio_codes)
    text = of_clip(text_states)
    live = lax.dynamic_index_in_dim(clip_weight[:, 0], clip, 0, False).astype(f32)
    length = lax.dynamic_slice_in_dim(text_length[:, 0], clip, 1)

    live_codes = fsdp_collect(jnp.where(live_mask, codes, -1))

    def chosen_entries(ids):
        return (ids[..., None] == table_ids).astype(bf16)

    embedded = row_sums(
        lambda ids: mm("ckfv,kdv->cfd", chosen_entries(ids), embed_tables),
        live_codes,
        axis=-1,
    )
    pieces = fsdp_exchange(embedded, -1, attn_ready)

    def place_of(block):
        place = 0
        for size, stride in fsdp_levels():
            gap = digit_of(block, size, stride) - digit_of(fsdp_index, size, stride)
            place = place * size + gap % size
        return place

    state_zero = jnp.concatenate(
        [lax.dynamic_index_in_dim(pieces, place_of(b), 0, False) for b in range(fsdp_count)], axis=1
    ) + positions(first_row, local_rows, D)

    rows_one = full_rows(layer_norm(state_zero, gains[0], gains[4]).astype(bf16))
    self_proj = [mm("fd,de->fe", rows_one, in_self[h]).astype(bf16) for h in halves]
    self_from = (0, cols, 2 * cols)
    lengths = (length, length + ffn_ready.astype(jnp.int32))
    mixed_one = [
        attend_forward((p, p, p), self_from, cols, n, True) for p, n in zip(self_proj, lengths)
    ]

    def project(left, right):
        return mm("fe,de->fd", left, right)

    def project_out(weights):
        return lambda a, b: project(a, weights[0]) + project(b, weights[1])

    state_one = state_zero + row_sums(project_out(out_self), *mixed_one)
    rows_two = full_rows(layer_norm(state_one, gains[1], gains[5]).astype(bf16))
    cross_query = [mm("fd,de->fe", rows_two, in_query[h]).astype(bf16) for h in halves]
    cross_kv = [mm("td,de->te", text, in_text[h]).astype(bf16) for h in halves]
    mixed_two = [
        attend_forward((q, kv, kv), (0, 0, cols), cols, length, False)
        for q, kv in zip(cross_query, cross_kv)
    ]
    state_two = state_one + row_sums(project_out(out_cross), *mixed_two)
    rows_three = full_rows(layer_norm(state_two, gains[2], gains[6]).astype(bf16))
    hidden_pre = [mm("fd,de->fe", rows_three, up[h]) for h in halves]
    active = [exact_gelu(a).astype(bf16) for a in hidden_pre]
    state_three = state_two + row_sums(project_out(down), *active)
    rows_four = full_rows(layer_norm(state_three, gains[3], gains[7]).astype(bf16))
    targets = jnp.concatenate([codes[:, 1:], jnp.zeros((BOOKS, 1), jnp.int32)], axis=1)
    logits = [mm("fd,kdv->kfv", rows_four, heads[h]) for h in halves]
    chosen = [targets[..., None] == half_ids[h] for h in halves]

    def half_stats(z, hit):
        top = jnp.max(z, axis=-1)
        mass = jnp.sum(jnp.exp(z - top[..., None]), axis=-1)
        picked = jnp.sum(jnp.where(hit, z, 0.0), axis=-1)
        return jnp.stack([top, mass, picked, jnp.sum(z, axis=-1)])

    stats = merge_stats(half_stats(logits[0], chosen[0]), half_stats(logits[1], chosen[1]))
    for bit in row_bits():
        stats = merge_stats(stats, tp_swap(stats, bit))
    log_total = stats[0] + jnp.log(stats[1])
    loss_terms = (
        log_total
        - (1.0 - smooth) * stats[2]
        - smooth * stats[3] / VOCAB
        + z_weight * log_total * log_total
    )
    numerator = live * jnp.sum(loss_terms * counted)
    row_scale = (live * counted)[..., None]

    def logit_gradient(z, hit):
        prob_rows = jnp.exp(z - log_total[..., None])
        return (
            row_scale
            * (
                prob_rows * (1.0 + 2.0 * z_weight * log_total[..., None])
                - (1.0 - smooth) * hit.astype(f32)
                - smooth / VOCAB
            )
        ).astype(bf16)

    grad_logits = [logit_gradient(logits[h], chosen[h]) for h in halves]

    def project_back(left, right):
        return mm("fd,de->fe", left, right)

    def weight_grad(left, right):
        return mm("fd,fe->de", left, right)

    grad_rows = row_sums(
        lambda a, b: mm("kfv,kdv->fd", a, heads[0]) + mm("kfv,kdv->fd", b, heads[1]), *grad_logits
    )
    def head_product(left, h):
        return mm("kfv,fd->kdv", grad_logits[h], left[0])

    def ffn_product(right):
        return lambda left, h: weight_grad(left[0], right[h])

    head_sum = across_last([rows_four], head_product, f16)
    next(head_sum)
    grad_state, gain_four, shift_four = norm_back(state_three, gains[3], grad_rows)

    grad_out = full_rows(grad_state.astype(bf16))
    grad_hidden = [
        gelu_back(hidden_pre[h], project_back(grad_out, down[h])).astype(bf16) for h in halves
    ]
    step, gain_three, shift_three = norm_back(
        state_two, gains[2], row_sums(project_out(up), *grad_hidden)
    )
    grad_three = grad_out
    up_sum = across_first([rows_three], ffn_product(grad_hidden), f16)
    down_sum = across_first([grad_three], ffn_product(active), f16)
    next(up_sum)
    next(down_sum)
    grad_state = grad_state + step

    grad_out = full_rows(grad_state.astype(bf16))
    grad_mixed = [project_back(grad_out, out_cross[h]).astype(bf16) for h in halves]
    grad_cross = [
        attend_backward((q, kv, kv, g), (0, 0, cols, 0), cols, length, False)
        for q, kv, g in zip(cross_query, cross_kv, grad_mixed)
    ]
    step, gain_two, shift_two = norm_back(
        state_one, gains[1], row_sums(project_out(in_query), *[g[0] for g in grad_cross])
    )
    grad_two = grad_out

    def cross_product(left, h):
        return jnp.concatenate(
            [
                weight_grad(left[0], grad_cross[h][0]),
                weight_grad(left[1], grad_cross[h][1]),
                weight_grad(left[1], grad_cross[h][2]),
                weight_grad(left[2], mixed_two[h]),
            ],
            axis=1,
        )

    cross_sum = across_last([rows_two, text, grad_two], cross_product, f16)
    next(cross_sum)
    head_sum.send(zero_of(gain_two))
    grad_state = grad_state + step

    grad_out = full_rows(grad_state.astype(bf16))
    grad_mixed = [project_back(grad_out, out_self[h]).astype(bf16) for h in halves]
    grad_self = [
        jnp.concatenate(attend_backward((p, p, p, g), self_from + (0,), cols, length, True), axis=1)
        for p, g in zip(self_proj, grad_mixed)
    ]
    step, gain_one, shift_one = norm_back(
        state_zero, gains[0], row_sums(project_out(in_self), *grad_self)
    )
    def self_product(left, h):
        return jnp.concatenate(
            [weight_grad(left[0], grad_self[h]), weight_grad(left[1], mixed_one[h])], axis=1
        )

    grad_one = grad_out
    self_sum = across_first([rows_one, grad_one], self_product, f16)
    next(self_sum)
    head_sum.send(zero_of(gain_one))
    grad_embed = (grad_state + step).astype(bf16)
    sent_blocks = jnp.stack(
        [
            lax.dynamic_slice_in_dim(grad_embed, o * shard_rows, shard_rows, axis=1)
            for o in shifted_all(fsdp_index, 1)
        ]
    )
    embed_rows = full_rows(fsdp_exchange(sent_blocks, 1), axis=1)
    came = zero_of(embed_rows)
    up_sum.send(came)
    down_sum.send(came)
    cross_sum.send(came)
    self_sum.send(came)
    head_grad = finish(head_sum, came)

    def table_part(h):
        hits = (live_codes[..., None] == half_ids[h]).astype(bf16)
        return mm("ckfv,cfd->kdv", hits, embed_rows)

    table_far = table_part(1)
    table_grad = table_part(0) + tp_swap(table_far, far)
    last = zero_of(table_far)
    for hop in (up_sum, down_sum, self_sum, cross_sum):
        hop.send(last)
    up_grad, down_grad, self_grad, cross_grad = [
        finish(hop, last) for hop in (up_sum, down_sum, self_sum, cross_sum)
    ]

    gain_total = jnp.stack(
        [gain_one, gain_two, gain_three, gain_four, shift_one, shift_two, shift_three, shift_four]
    )
    for bit in row_bits() + [far]:
        gain_total = gain_total + tp_swap(gain_total, bit)
    gain_grad = fsdp_scatter(gain_total[..., None])[..., 0]

    only_first = (tp_index == 0).astype(f32)
    once = (tp_index % far == 0).astype(f32)
    kept_squares = jnp.sum(table_grad * table_grad) + only_first * jnp.sum(gain_grad * gain_grad)
    lanes = jnp.arange(PAIR)[None, :] + jnp.zeros((8, 1), jnp.int32)

    def totals(*values):
        sums = jnp.zeros((8, PAIR), f32)
        for lane, value in enumerate(values):
            sums = jnp.where(lanes == lane, value, sums)
        return everywhere(jnp.add, sums, row_bits() + [far])[0]

    def squares(*grads):
        return [jnp.sum(g * g) for g in grads]

    wired = (head_grad, up_grad, down_grad, cross_grad, self_grad)
    sums = totals(kept_squares, numerator * once, live * once, *squares(*wired))
    group_sums = sums[3:8]

    devices = float(fsdp_count * 2 * far)
    counts = jnp.array([g.size * devices for g in wired], f32)
    fits = jnp.isfinite(jnp.sum(group_sums)) & jnp.all(group_sums >= counts * 2.0**-30)

    def as_sent():
        return wired + (jnp.sum(group_sums),)

    def again():
        groups = (
            across_last([rows_four], head_product, f32),
            across_first([rows_three], ffn_product(grad_hidden), f32),
            across_first([grad_three], ffn_product(active), f32),
            across_last([rows_two, text, grad_two], cross_product, f32),
            across_first([rows_one, grad_one], self_product, f32),
        )
        grads = []
        for group in groups:
            next(group)
            grads.append(finish(group))
        return tuple(grads) + (totals(sum(squares(*grads)))[0],)

    head_grad, up_grad, down_grad, cross_grad, self_grad, group_total = lax.cond(
        fits, as_sent, again
    )
    vocab_grad = jnp.stack([table_grad, head_grad])
    self_parts = jnp.split(self_grad, 4, axis=1)
    cross_parts = jnp.split(cross_grad, 4, axis=1)
    attn_grad = jnp.stack(
        self_parts[:3] + cross_parts[:3] + [self_parts[3], cross_parts[3]], axis=0
    )
    ffn_grad = jnp.stack([up_grad, down_grad])
    per_clip = BOOKS * (frames - 1) - BOOKS * (BOOKS - 1) // 2
    counted_total = sums[2] * per_clip
    step_loss = sums[1] / counted_total
    grad_norm = jnp.sqrt(sums[0] + group_total)
    factor = jnp.minimum(1.0, clip_scale * jnp.sqrt(counted_total) / (grad_norm + 1e-06))
    step_float = step_count[0].astype(f32)
    vocab_out = adam_update(vocab_tables, vocab_grad, vocab_m, vocab_v, factor, step_float, True)
    attn_out = adam_update(attn_weights, attn_grad, attn_m, attn_v, factor, step_float, True)
    ffn_out = adam_update(ffn_weights, ffn_grad, ffn_m, ffn_v, factor, step_float, True)
    norm_out = adam_update(norm_params, gain_grad, norm_m, norm_v, factor, step_float, False)
    return (step_loss, grad_norm) + vocab_out + attn_out + ffn_out + norm_out


def solution(mesh):
    batch = P(None, "fsdp")
    clip = P(None, "fsdp", None, None)
    table = P(None, None, "fsdp", "tp")
    matrix = P(None, "fsdp", "tp")
    placed = (clip, clip, batch, batch, P(), table, matrix, matrix, batch)
    moments = (table, table, matrix, matrix, matrix, matrix, batch, batch)
    return jax.shard_map(
        per_device,
        mesh=mesh,
        in_specs=placed + moments,
        out_specs=(P(), P()) + (table,) * 4 + (matrix,) * 8 + (batch,) * 4,
        check_vma=False,
    )
```
